32 devices in a mesh: groups: 2 (over x), seq: 8 (over z, y), head: 2 (over core).
Axes of the slice: x: 2, y: 2, z: 4, core: 2. Of those that a mesh axis runs over, the one named last changes fastest.
Arguments:
- queries: bfloat16 [2048, 28, 128], P(('groups', 'seq'), 'head'), parts along dimension 0, may hold values from -400 to 400, as said below
- request_image: int32 [2048, 1], P(('groups', 'seq')), parts along dimension 0, may hold values from 0 to 15; in each aligned block of 128 rows (0 to 127, 128 to 255, ...) at most 16 rows name the same one
- image_slot: int32 [32], P('groups'), parts along dimension 0, may hold values from 0 to 15, each once
- image_lengths: int32 [32], P(('groups', 'seq')), parts along dimension 0, may hold values from 640 to 1280
- image_keys: bfloat16 [32, 4, 1280, 128], P(('groups', 'seq'), 'head'), parts along dimension 0, may hold values from -6 to 6
- image_values: bfloat16 [32, 4, 1280, 128], P(('groups', 'seq'), 'head'), parts along dimension 0, may hold values from -6 to 6
- text_keys: bfloat16 [2048, 4, 64, 128], P(('groups', 'seq'), 'head'), parts along dimension 0, may hold values from -6 to 6
- text_values: bfloat16 [2048, 4, 64, 128], P(('groups', 'seq'), 'head'), parts along dimension 0, may hold values from -6 to 6
- text_lengths: int32 [2048], P(('groups', 'seq')), parts along dimension 0, may hold values from 1 to 64
Outputs:
- attention: bfloat16 [2048, 28, 128], P(('groups', 'seq'), 'head'), parts along dimension 0
The draws below stay inside these ranges and needn't reach their ends.
There are 2 independent parts, one for each index of `groups`. The reference program is written for one: setup_inputs(seed, part) draws one part's arguments, and reference() takes and returns one part's arrays. A program takes and returns all parts, laid end to end along the dimension named above; each array names one. Nothing has to cross between parts.
Inputs may be any that keep to these rules, and one draw needn't show every extreme that they name: queries are finite bfloat16 values. `request_image`: the requests of one index of seq name any one image at most 16 times, and in some index of seq some image is named exactly 16 times. `image_slot`: a permutation; the image in storage slot s is held by index s // 2 of seq.
All inputs are finite; a program needn't handle non-finite values.
Results may differ from the reference program's by a relative error of at most 0.0056.
Values may be sent and summed in bfloat16 or wider, within the bound.
No kernel may reach another device: no remote copies, remote signals or barrier semaphores. Data moves between devices by JAX's collectives and lax.ppermute only.
A program may use at most 64 MiB of HBM per device.

```python
import math
import jax
import jax.numpy as jnp
import numpy as np
from jax import lax

D_HEAD = 128
KV_HEADS = 4
Q_HEADS = 28
IMG_TOK = 1280
TXT_TOK = 64
REQ_DEV = 128
REQUESTS = 1024
IMAGES = 16
MOST = 16


def draw_queries(key, part):
    base = jax.random.truncated_normal(key, -6.0, 6.0, (REQUESTS, Q_HEADS, D_HEAD), jnp.float32)
    return base.astype(jnp.bfloat16)


def touch_ends(drawn, own_key, smallest, high):
    spot = [jax.random.randint(jax.random.fold_in(own_key, axis), (), 0, length) for axis, length in enumerate(drawn.shape)]
    longest = drawn.shape.index(max(drawn.shape))
    neighbour = spot[:longest] + [(spot[longest] + 1) % drawn.shape[longest]] + spot[longest + 1:]
    return drawn.at[tuple(spot)].set(smallest).at[tuple(neighbour)].set(high)


def level_of(rng, extent, shards, smallest, largest):
    level, own = 1.0, jax.random.fold_in(rng, 6)
    for axis_at, shards_of in shards:
        steps = jnp.exp(jax.random.uniform(jax.random.fold_in(own, axis_at), (shards_of,), jnp.float32, smallest / len(shards), largest / len(shards)))
        level = level * jnp.repeat(steps, extent[axis_at] // shards_of).reshape([-1 if axis == axis_at else 1 for axis in range(len(extent))])
    return level


def routed_block(rng, own, number, rows, amount, top, limit, slope):
    ranking = jax.random.permutation(rng, amount)
    crowded, ordinary = portions_of(amount, rows * top, limit, slope, True), portions_of(amount, rows * top, limit, slope, False)
    places = jnp.arange(amount)

    def named(lengths, rotation):
        used = int((lengths > 0).sum())
        fixed = max(1, used // 4)
        passed = fixed + (places - fixed + rotation * (used - fixed)) % max(1, amount - fixed)
        return jnp.zeros((amount,), jnp.int32).at[ranking[jnp.where(places < fixed, places, passed)]].set(jnp.asarray(lengths, jnp.int32))

    lengths = jnp.where(number % 4 == 0, named(crowded, number // 4), named(ordinary, number - number // 4 - 1))
    mixed = jax.random.permutation(jax.random.fold_in(own, 3), amount)
    source_of, receiver = mixed[0:amount // 2 * 2:2], mixed[1:amount // 2 * 2:2]
    slack = jnp.minimum(lengths[source_of] - 1, limit - lengths[receiver]) // 2
    slack = jnp.where((source_of == ranking[0]) | (receiver == ranking[0]) | (lengths[receiver] == 0), 0, jnp.maximum(slack, 0))
    passed = jax.random.randint(jax.random.fold_in(own, 4), (amount // 2,), 0, 1 << 20) % (slack + 1)
    lengths = lengths.at[source_of].add(-passed).at[receiver].add(passed)
    members = jnp.searchsorted(jnp.cumsum(lengths), jnp.arange(rows * top), side="right").astype(jnp.int32)
    grid = members.reshape(top, rows).T
    grid = grid[jax.random.permutation(jax.random.fold_in(own, 1), rows)]
    rotation = jax.random.randint(jax.random.fold_in(own, 2), (rows, 1), 0, top)
    return jnp.take_along_axis(grid, (jnp.arange(top)[None, :] + rotation) % top, axis=1)


def portions_of(number_of, total, reach, slope, full):
    weights = [(1 << 20) // math.isqrt(grade ** slope) + 1 for grade in range(1, number_of + 1)]
    largest = reach if full else min(reach, max(-(-total // number_of), total * weights[0] // sum(weights)))
    least = 1 if total - largest >= number_of - 1 else 0
    given, spare = [largest] + [least] * (number_of - 1), total - largest - least * (number_of - 1)
    while spare > 0:
        candidates = [i for i in range(1, number_of) if given[i] < largest] or [i for i in range(1, number_of) if given[i] < reach]
        whole, remaining = sum([weights[i] for i in candidates]), spare
        for i in candidates:
            extra = min(reach - given[i], max(1, remaining * weights[i] // whole), spare)
            given[i] = given[i] + extra
            spare = spare - extra
    return np.array(given)


def scatter_about(key, extent, deviation, reach, split=(), held_as=jnp.bfloat16):
    result = deviation * jax.random.normal(key, extent, jnp.float32)
    if split:
        result = result * level_of(key, extent, split, -0.22, 0.18)
    return jnp.clip(result, -reach, reach).astype(held_as)


def setup_inputs(seed: int = 0, part: int = 0) -> dict:
    key_of = jax.random.split(jax.random.key(seed), 10)
    part_splits = jax.random.split(jax.random.fold_in(key_of[9], part), 10)
    queries = draw_queries(jax.random.fold_in(jax.random.fold_in(key_of[9], part), 71), part)
    request_image_keys = jax.random.split(jax.random.fold_in(part_splits[1], 1), REQUESTS // REQ_DEV)
    request_image_turns = jax.random.permutation(jax.random.fold_in(part_splits[1], 3), REQUESTS // REQ_DEV)
    request_image = jax.vmap(lambda own, number: routed_block(jax.random.fold_in(part_splits[1], 2), own, number, REQ_DEV, IMAGES, 1, MOST, 2))(request_image_keys, request_image_turns).reshape((REQUESTS, 1))
    image_slot = jax.random.permutation(part_splits[2], IMAGES).astype(jnp.int32)
    image_lengths = touch_ends(jax.random.randint(part_splits[3], (IMAGES,), IMG_TOK // 2, IMG_TOK + 1), jax.random.fold_in(part_splits[3], 1), IMG_TOK // 2, IMG_TOK).astype(jnp.int32)
    image_keys = scatter_about(part_splits[4], (IMAGES, KV_HEADS, IMG_TOK, D_HEAD), 1.0, 6.0, ((0, 8), (1, 2)))
    image_values = scatter_about(part_splits[5], (IMAGES, KV_HEADS, IMG_TOK, D_HEAD), 1.0, 6.0, ((0, 8), (1, 2)))
    text_keys = scatter_about(part_splits[6], (REQUESTS, KV_HEADS, TXT_TOK, D_HEAD), 1.0, 6.0, ((0, 8), (1, 2)))
    text_values = scatter_about(part_splits[7], (REQUESTS, KV_HEADS, TXT_TOK, D_HEAD), 1.0, 6.0, ((0, 8), (1, 2)))
    text_lengths = touch_ends(jax.random.randint(part_splits[8], (REQUESTS,), 1, TXT_TOK + 1), jax.random.fold_in(part_splits[8], 1), 1, TXT_TOK).astype(jnp.int32)
    return dict(queries=queries, request_image=request_image, image_slot=image_slot, image_lengths=image_lengths, image_keys=image_keys, image_values=image_values, text_keys=text_keys, text_values=text_values, text_lengths=text_lengths)


NEGATIVE = -1e+30

def partial_attend(query_heads, keys, values, valid, scale):
    scores = jnp.einsum('bhgd,bhtd->bhgt', query_heads, keys) * scale
    scores = jnp.where(valid, scores, NEGATIVE)
    highest = lax.optimization_barrier(jnp.max(scores, axis=-1, keepdims=True))
    weights = jnp.where(valid, jnp.exp(scores - highest), 0.0)
    total = lax.optimization_barrier(jnp.sum(weights, axis=-1, keepdims=True))
    rounded = lax.optimization_barrier(weights.astype(jnp.bfloat16)).astype(jnp.float32)
    output = jnp.einsum('bhgt,bhtd->bhgd', rounded, values) / total
    return (output, highest[..., 0] + jnp.log(total[..., 0]))

def merge_parts(image_out, image_lse, text_out, text_lse):
    highest = jnp.maximum(image_lse, text_lse)
    image_weight = jnp.exp(image_lse - highest)[..., None]
    text_weight = jnp.exp(text_lse - highest)[..., None]
    return (image_weight * image_out + text_weight * text_out) / (image_weight + text_weight)

def reference(queries, request_image, image_slot, image_lengths, image_keys, image_values, text_keys, text_values, text_lengths):
    scale = 1.0 / math.sqrt(D_HEAD)
    group = Q_HEADS // KV_HEADS
    slots = image_slot[request_image[:, 0]].astype(jnp.int32)
    blocks = REQUESTS // REQ_DEV

    def one_block(packed):
        block_queries, block_slots, block_tkeys, block_tvalues, block_tlen = packed
        query_heads = block_queries.astype(jnp.float32).reshape(REQ_DEV, KV_HEADS, group, D_HEAD)
        keys = image_keys[block_slots].astype(jnp.float32)
        values = image_values[block_slots].astype(jnp.float32)
        image_valid = (jnp.arange(IMG_TOK, dtype=jnp.int32)[None, :] < image_lengths[block_slots][:, None])[:, None, None, :]
        image_out, image_lse = partial_attend(query_heads, keys, values, image_valid, scale)
        image_out = lax.optimization_barrier(image_out.astype(jnp.bfloat16)).astype(jnp.float32)
        text_valid = (jnp.arange(TXT_TOK, dtype=jnp.int32)[None, :] < block_tlen[:, None])[:, None, None, :]
        text_out, text_lse = partial_attend(query_heads, block_tkeys.astype(jnp.float32), block_tvalues.astype(jnp.float32), text_valid, scale)
        merged = merge_parts(image_out, image_lse, text_out, text_lse)
        return merged.reshape(REQ_DEV, Q_HEADS, D_HEAD).astype(jnp.bfloat16)
    packed = (queries.reshape(blocks, REQ_DEV, Q_HEADS, D_HEAD), slots.reshape(blocks, REQ_DEV), text_keys.reshape(blocks, REQ_DEV, KV_HEADS, TXT_TOK, D_HEAD), text_values.reshape(blocks, REQ_DEV, KV_HEADS, TXT_TOK, D_HEAD), text_lengths.reshape(blocks, REQ_DEV))
    return lax.map(one_block, packed).reshape(REQUESTS, Q_HEADS, D_HEAD)
```

```python
import functools
import math

import jax
import jax.numpy as jnp
from jax import lax
from jax.experimental import pallas as pl
from jax.experimental.pallas import tpu as pltpu
from jax.sharding import PartitionSpec as P

NEGATIVE = -1e30


def weigh(scores, valid):
    scores = jnp.where(valid, scores, NEGATIVE)
    highest = jnp.max(scores, axis=-1, keepdims=True)
    weights = jnp.where(valid, jnp.exp(scores - highest), 0.0)
    total = jnp.sum(weights, axis=-1, keepdims=True)
    return (weights.astype(jnp.bfloat16), total, highest)

LANES = 128
PIECES = 3


def image_body(lengths, queries, keys, values, out, *, group, scale):
    sources, count, _ = queries.shape
    local_kv, tokens, head_size = keys.shape
    rows = sources * count
    index = pl.program_id(0)
    length = lengths[index]
    factor = scale * math.log2(math.e)
    valid = lax.broadcasted_iota(jnp.int32, (tokens, head_size), 0) < length
    lane = lax.broadcasted_iota(jnp.int32, (rows, LANES), 1)
    local_heads = local_kv * group
    lse_all = jnp.zeros((rows, LANES), jnp.float32)
    ones = jnp.where(valid, 1.0, 0.0).astype(jnp.bfloat16)
    for kv in range(local_kv):
        kept = keys[kv].astype(jnp.float32)
        kept = jnp.where(valid, kept, kept[0:1]).astype(jnp.bfloat16)
        value = jnp.where(valid, values[kv].astype(jnp.float32), 0.0).astype(jnp.bfloat16)
        value = jnp.concatenate([value, ones], axis=1)
        start = 0
        while start < group:
            take = 2 if group - start != 3 else 3
            take = min(take, group - start)
            heads = [kv * group + start + j for j in range(take)]
            block = jnp.concatenate(
                [
                    queries[:, :, h * head_size : (h + 1) * head_size].reshape(rows, head_size)
                    for h in heads
                ],
                axis=0,
            )
            scores = lax.dot_general(
                block, kept, (((1,), (1,)), ((), ())), preferred_element_type=jnp.float32
            )
            highest = jnp.max(scores, axis=1, keepdims=True)
            weights = jnp.exp2((scores - highest) * factor).astype(jnp.bfloat16)
            summed = jnp.dot(weights, value, preferred_element_type=jnp.float32)
            total = summed[:, head_size:]
            result = (summed[:, :head_size] / total).astype(jnp.bfloat16)
            lse = highest * scale + jnp.log(total)
            for j, h in enumerate(heads):
                out[:, :, h * head_size : (h + 1) * head_size] = result[
                    j * rows : (j + 1) * rows
                ].reshape(sources, count, head_size)
                lse_all = jnp.where(lane % local_heads == h, lse[j * rows : (j + 1) * rows], lse_all)
            start += take
    high = lse_all.astype(jnp.bfloat16).astype(jnp.float32)
    middle = (lse_all - high).astype(jnp.bfloat16).astype(jnp.float32)
    low = lse_all - high - middle
    piece = jnp.where(lane < local_heads, high, jnp.where(lane < 2 * local_heads, middle, low))
    width = local_heads * head_size
    out[:, :, width : width + LANES] = piece.astype(jnp.bfloat16).reshape(sources, count, LANES)


def attend_images(incoming, image_keys, image_values, image_lengths, group, scale):
    sources, held, count, width = incoming.shape
    if count % 16:
        incoming = incoming.transpose(1, 0, 2, 3).reshape(1, held, sources * count, width)
    lead, _, inner, _ = incoming.shape
    _, local_kv, tokens, head_size = image_keys.shape
    wide = width + LANES
    cache = pl.BlockSpec((None, local_kv, tokens, head_size), lambda i: (i, 0, 0, 0))
    out = pl.pallas_call(
        functools.partial(image_body, group=group, scale=scale),
        grid=(held,),
        in_specs=[
            pl.BlockSpec(memory_space=pltpu.SMEM),
            pl.BlockSpec((lead, None, inner, width), lambda i: (0, i, 0, 0)),
            cache,
            cache,
        ],
        out_specs=pl.BlockSpec((lead, None, inner, wide), lambda i: (0, i, 0, 0)),
        out_shape=jax.ShapeDtypeStruct((lead, held, inner, wide), jnp.bfloat16),
        compiler_params=pltpu.CompilerParams(vmem_limit_bytes=48 * 1024 * 1024),
        name="image_attention",
    )(image_lengths, incoming, image_keys, image_values)
    if count % 16:
        out = out.reshape(held, sources, count, wide).transpose(1, 0, 2, 3)
    return out


def on_device(
    queries,
    request_image,
    image_slot,
    image_lengths,
    image_keys,
    image_values,
    text_keys,
    text_values,
    text_lengths,
):
    rows, local_heads, head_size = queries.shape
    local_kv = image_keys.shape[1]
    group = local_heads // local_kv
    images = image_slot.shape[0]
    held = image_keys.shape[0]
    image_tokens = image_keys.shape[2]
    text_tokens = text_keys.shape[2]
    devices = lax.axis_size("seq")
    most = max(2, 2 * rows // images)
    width = local_heads * head_size
    scale = 1.0 / math.sqrt(head_size)
    image_ids = jnp.arange(images, dtype=jnp.int32)
    chosen = request_image == image_ids[None, :]
    slots = jnp.sum(jnp.where(chosen, image_slot[None, :], 0), axis=1)
    slot_hits = (slots[:, None] == image_ids[None, :]).astype(jnp.int32)
    ranks = jnp.sum(slot_hits * (jnp.cumsum(slot_hits, axis=0) - 1), axis=1)
    targets = slots * most + ranks
    dispatch = (jnp.arange(images * most, dtype=jnp.int32)[:, None] == targets[None, :]).astype(
        jnp.bfloat16
    )
    flat_queries = queries.reshape(rows, width)
    outgoing = jnp.dot(dispatch, flat_queries, preferred_element_type=jnp.float32).astype(
        jnp.bfloat16
    )
    outgoing = outgoing.reshape(devices, held, most, width)
    incoming = lax.all_to_all(outgoing, "seq", split_axis=0, concat_axis=0, tiled=True)
    stacked = attend_images(incoming, image_keys, image_values, image_lengths, group, scale)
    back = lax.all_to_all(stacked, "seq", split_axis=0, concat_axis=0, tiled=True)
    flat_back = back.reshape(images * most, width + LANES)
    fetched = jnp.einsum("sr,sc->rc", dispatch, flat_back, preferred_element_type=jnp.float32)
    image_part = fetched[:, :width].reshape(rows, local_kv, group, head_size)
    pieces = fetched[:, width : width + PIECES * local_heads]
    image_lse = jnp.sum(pieces.reshape(rows, PIECES, local_heads), axis=1)
    image_lse = image_lse.reshape(rows, local_kv, group)
    heads = queries.reshape(rows, local_kv, group, head_size)
    scores = (
        jnp.einsum("rhgd,rhtd->rhgt", heads, text_keys, preferred_element_type=jnp.float32) * scale
    )
    valid = (jnp.arange(text_tokens, dtype=jnp.int32)[None, :] < text_lengths[:, None])[
        :, None, None, :
    ]
    weights, total, highest = weigh(scores, valid)
    text_out = (
        jnp.einsum("rhgt,rhtd->rhgd", weights, text_values, preferred_element_type=jnp.float32)
        / total
    )
    text_lse = highest[..., 0] + jnp.log(total[..., 0])
    upper = jnp.maximum(image_lse, text_lse)
    image_weight = jnp.exp(image_lse - upper)[..., None]
    text_weight = jnp.exp(text_lse - upper)[..., None]
    merged = (image_weight * image_part + text_weight * text_out) / (image_weight + text_weight)
    return merged.reshape(rows, local_heads, head_size).astype(jnp.bfloat16)


def solution(mesh):
    in_specs = (
        P(("groups", "seq"), "head", None),
        P(("groups", "seq"), None),
        P("groups"),
        P(("groups", "seq")),
        P(("groups", "seq"), "head", None, None),
        P(("groups", "seq"), "head", None, None),
        P(("groups", "seq"), "head", None, None),
        P(("groups", "seq"), "head", None, None),
        P(("groups", "seq")),
    )
    out_specs = P(("groups", "seq"), "head", None)
    return jax.shard_map(
        on_device, mesh=mesh, in_specs=in_specs, out_specs=out_specs, check_vma=False
    )
```

```python
import functools
import math

import jax
import jax.numpy as jnp
from jax import lax
from jax.experimental import pallas as pl
from jax.experimental.pallas import tpu as pltpu
from jax.sharding import PartitionSpec as P

NEGATIVE = -1e30


def weigh(scores, valid):
    scores = jnp.where(valid, scores, NEGATIVE)
    highest = jnp.max(scores, axis=-1, keepdims=True)
    weights = jnp.where(valid, jnp.exp(scores - highest), 0.0)
    total = jnp.sum(weights, axis=-1, keepdims=True)
    return (weights.astype(jnp.bfloat16), total, highest)

LANES = 128
PIECES = 3


def image_body(lengths, queries, keys, values, out, *, group, scale):
    sources, count, _ = queries.shape
    local_kv, tokens, head_size = keys.shape
    rows = sources * count
    index = pl.program_id(0)
    length = lengths[index]
    factor = scale * math.log2(math.e)
    valid = lax.broadcasted_iota(jnp.int32, (tokens, head_size), 0) < length
    lane = lax.broadcasted_iota(jnp.int32, (rows, LANES), 1)
    local_heads = local_kv * group
    lse_all = jnp.zeros((rows, LANES), jnp.float32)
    ones = jnp.where(valid, 1.0, 0.0).astype(jnp.bfloat16)
    for kv in range(local_kv):
        kept = keys[kv].astype(jnp.float32)
        kept = jnp.where(valid, kept, kept[0:1]).astype(jnp.bfloat16)
        value = jnp.where(valid, values[kv].astype(jnp.float32), 0.0).astype(jnp.bfloat16)
        value = jnp.concatenate([value, ones], axis=1)
        start = 0
        while start < group:
            take = 2 if group - start != 3 else 3
            take = min(take, group - start)
            heads = [kv * group + start + j for j in range(take)]
            block = jnp.concatenate(
                [
                    queries[:, :, h * head_size : (h + 1) * head_size].reshape(rows, head_size)
                    for h in heads
                ],
                axis=0,
            )
            scores = lax.dot_general(
                block, kept, (((1,), (1,)), ((), ())), preferred_element_type=jnp.float32
            )
            highest = jnp.max(scores, axis=1, keepdims=True)
            weights = jnp.exp2((scores - highest) * factor).astype(jnp.bfloat16)
            summed = jnp.dot(weights, value, preferred_element_type=jnp.float32)
            total = summed[:, head_size:]
            result = (summed[:, :head_size] / total).astype(jnp.bfloat16)
            lse = highest * scale + jnp.log(total)
            for j, h in enumerate(heads):
                out[:, :, h * head_size : (h + 1) * head_size] = result[
                    j * rows : (j + 1) * rows
                ].reshape(sources, count, head_size)
                lse_all = jnp.where(lane % local_heads == h, lse[j * rows : (j + 1) * rows], lse_all)
            start += take
    high = lse_all.astype(jnp.bfloat16).astype(jnp.float32)
    middle = (lse_all - high).astype(jnp.bfloat16).astype(jnp.float32)
    low = lse_all - high - middle
    piece = jnp.where(lane < local_heads, high, jnp.where(lane < 2 * local_heads, middle, low))
    width = local_heads * head_size
    out[:, :, width : width + LANES] = piece.astype(jnp.bfloat16).reshape(sources, count, LANES)


def attend_images(incoming, image_keys, image_values, image_lengths, group, scale):
    sources, held, count, width = incoming.shape
    if count % 16:
        incoming = incoming.transpose(1, 0, 2, 3).reshape(1, held, sources * count, width)
    lead, _, inner, _ = incoming.shape
    _, local_kv, tokens, head_size = image_keys.shape
    wide = width + LANES
    cache = pl.BlockSpec((None, local_kv, tokens, head_size), lambda i: (i, 0, 0, 0))
    out = pl.pallas_call(
        functools.partial(image_body, group=group, scale=scale),
        grid=(held,),
        in_specs=[
            pl.BlockSpec(memory_space=pltpu.SMEM),
            pl.BlockSpec((lead, None, inner, width), lambda i: (0, i, 0, 0)),
            cache,
            cache,
        ],
        out_specs=pl.BlockSpec((lead, None, inner, wide), lambda i: (0, i, 0, 0)),
        out_shape=jax.ShapeDtypeStruct((lead, held, inner, wide), jnp.bfloat16),
        compiler_params=pltpu.CompilerParams(vmem_limit_bytes=48 * 1024 * 1024),
        name="image_attention",
    )(image_lengths, incoming, image_keys, image_values)
    if count % 16:
        out = out.reshape(held, sources, count, wide).transpose(1, 0, 2, 3)
    return out


def prepare_body(request_image, image_slot, queries, outgoing, targets, *, most):
    local_heads, rows, _ = queries.shape
    images = image_slot.shape[1]
    ids = lax.broadcasted_iota(jnp.int32, (rows, images), 1)
    slot_values = jnp.where(request_image[...] == ids, image_slot[...], 0).astype(jnp.float32)
    slots = jnp.sum(slot_values, axis=1, keepdims=True)
    hits = jnp.where(ids.astype(jnp.float32) == slots, 1.0, 0.0)
    earlier = lax.broadcasted_iota(jnp.int32, (rows, rows), 1) < lax.broadcasted_iota(
        jnp.int32, (rows, rows), 0
    )
    before = jnp.dot(
        jnp.where(earlier, 1.0, 0.0).astype(jnp.bfloat16),
        hits.astype(jnp.bfloat16),
        preferred_element_type=jnp.float32,
    )
    ranks = jnp.sum(hits * before, axis=1, keepdims=True)
    places = (slots * most + ranks).astype(jnp.int32)
    targets[...] = places
    columns = lax.broadcasted_iota(jnp.int32, (rows, images * most), 1)
    dispatch = jnp.where(columns == places, 1.0, 0.0).astype(jnp.bfloat16)
    flat = jnp.concatenate([queries[h] for h in range(local_heads)], axis=1)
    outgoing[...] = lax.dot_general(
        dispatch, flat, (((0,), (0,)), ((), ())), preferred_element_type=jnp.float32
    ).astype(jnp.bfloat16)


def prepare(request_image, image_slot, queries, most):
    rows, local_heads, head_size = queries.shape
    images = image_slot.shape[0]
    return pl.pallas_call(
        functools.partial(prepare_body, most=most),
        out_shape=(
            jax.ShapeDtypeStruct((images * most, local_heads * head_size), jnp.bfloat16),
            jax.ShapeDtypeStruct((rows, 1), jnp.int32),
        ),
        compiler_params=pltpu.CompilerParams(vmem_limit_bytes=16 * 1024 * 1024),
        name="prepare",
    )(request_image, image_slot.reshape(1, images), queries.transpose(1, 0, 2))


def merge_body(targets, back, text, text_lse, out):
    local_heads, rows, head_size = out.shape
    places = back.shape[0]
    width = local_heads * head_size
    columns = lax.broadcasted_iota(jnp.int32, (rows, places), 1)
    dispatch = jnp.where(columns == targets[...], 1.0, 0.0).astype(jnp.bfloat16)
    pieces = jnp.dot(dispatch, back[:, width:], preferred_element_type=jnp.float32)
    source = lax.broadcasted_iota(jnp.int32, (LANES, LANES), 0)
    target = lax.broadcasted_iota(jnp.int32, (LANES, LANES), 1)
    joined = (source == target) & (target < local_heads)
    for piece in range(1, PIECES):
        joined = joined | ((source == target + piece * local_heads) & (target < local_heads))
    image_lse = jnp.dot(
        pieces.astype(jnp.bfloat16),
        jnp.where(joined, 1.0, 0.0).astype(jnp.bfloat16),
        preferred_element_type=jnp.float32,
    )[:, :local_heads]
    upper = jnp.maximum(image_lse, text_lse[...])
    image_weight = jnp.exp(image_lse - upper)
    share = image_weight / (image_weight + jnp.exp(text_lse[...] - upper))
    image = jnp.dot(dispatch, back[:, :width], preferred_element_type=jnp.float32)
    for h in range(local_heads):
        own = text[h]
        part = image[:, h * head_size : (h + 1) * head_size]
        out[h] = (own + share[:, h : h + 1] * (part - own)).astype(jnp.bfloat16)


def merge(targets, back, text, text_lse, local_heads):
    rows = targets.shape[0]
    head_size = text.shape[2]
    return pl.pallas_call(
        merge_body,
        out_shape=jax.ShapeDtypeStruct((local_heads, rows, head_size), jnp.bfloat16),
        compiler_params=pltpu.CompilerParams(vmem_limit_bytes=16 * 1024 * 1024),
        name="merge",
    )(targets, back, text, text_lse).transpose(1, 0, 2)


def on_device(
    queries,
    request_image,
    image_slot,
    image_lengths,
    image_keys,
    image_values,
    text_keys,
    text_values,
    text_lengths,
):
    rows, local_heads, head_size = queries.shape
    local_kv = image_keys.shape[1]
    group = local_heads // local_kv
    images = image_slot.shape[0]
    held = image_keys.shape[0]
    image_tokens = image_keys.shape[2]
    text_tokens = text_keys.shape[2]
    devices = lax.axis_size("seq")
    most = max(2, 2 * rows // images)
    width = local_heads * head_size
    scale = 1.0 / math.sqrt(head_size)
    outgoing, targets = prepare(request_image, image_slot, queries, most)
    outgoing = outgoing.reshape(devices, held, most, width)
    incoming = lax.all_to_all(outgoing, "seq", split_axis=0, concat_axis=0, tiled=True)
    stacked = attend_images(incoming, image_keys, image_values, image_lengths, group, scale)
    back = lax.all_to_all(stacked, "seq", split_axis=0, concat_axis=0, tiled=True)
    flat_back = back.reshape(images * most, width + LANES)
    heads = queries.reshape(rows, local_kv, group, head_size)
    scores = (
        jnp.einsum("rhgd,rhtd->rhgt", heads, text_keys, preferred_element_type=jnp.float32) * scale
    )
    valid = (jnp.arange(text_tokens, dtype=jnp.int32)[None, :] < text_lengths[:, None])[
        :, None, None, :
    ]
    weights, total, highest = weigh(scores, valid)
    text_out = (
        jnp.einsum("rhgt,rhtd->rhgd", weights, text_values, preferred_element_type=jnp.float32)
        / total
    )
    text_lse = highest[..., 0] + jnp.log(total[..., 0])
    text_flat = text_out.reshape(rows, local_heads, head_size).transpose(1, 0, 2)
    return merge(targets, flat_back, text_flat, text_lse.reshape(rows, local_heads), local_heads)


def solution(mesh):
    in_specs = (
        P(("groups", "seq"), "head", None),
        P(("groups", "seq"), None),
        P("groups"),
        P(("groups", "seq")),
        P(("groups", "seq"), "head", None, None),
        P(("groups", "seq"), "head", None, None),
        P(("groups", "seq"), "head", None, None),
        P(("groups", "seq"), "head", None, None),
        P(("groups", "seq")),
    )
    out_specs = P(("groups", "seq"), "head", None)
    return jax.shard_map(
        on_device, mesh=mesh, in_specs=in_specs, out_specs=out_specs, check_vma=False
    )
```

```python
import functools
import math

import jax
import jax.numpy as jnp
from jax import lax
from jax.experimental import pallas as pl
from jax.experimental.pallas import tpu as pltpu
from jax.sharding import PartitionSpec as P

NEGATIVE = -1e30


def weigh(scores, valid):
    scores = jnp.where(valid, scores, NEGATIVE)
    highest = jnp.max(scores, axis=-1, keepdims=True)
    weights = jnp.where(valid, jnp.exp(scores - highest), 0.0)
    total = jnp.sum(weights, axis=-1, keepdims=True)
    return (weights.astype(jnp.bfloat16), total, highest)

LANES = 128
PIECES = 3


def image_body(lengths, queries, keys, values, out, *, group, scale):
    sources, count, _ = queries.shape
    local_kv, tokens, head_size = keys.shape
    rows = sources * count
    index = pl.program_id(0)
    length = lengths[index]
    factor = scale * math.log2(math.e)
    valid = lax.broadcasted_iota(jnp.int32, (tokens, head_size), 0) < length
    lane = lax.broadcasted_iota(jnp.int32, (rows, LANES), 1)
    local_heads = local_kv * group
    lse_all = jnp.zeros((rows, LANES), jnp.float32)
    ones = jnp.where(valid, 1.0, 0.0).astype(jnp.bfloat16)
    for kv in range(local_kv):
        kept = keys[kv].astype(jnp.float32)
        kept = jnp.where(valid, kept, kept[0:1]).astype(jnp.bfloat16)
        value = jnp.where(valid, values[kv].astype(jnp.float32), 0.0).astype(jnp.bfloat16)
        value = jnp.concatenate([value, ones], axis=1)
        start = 0
        while start < group:
            take = 2 if group - start != 3 else 3
            take = min(take, group - start)
            heads = [kv * group + start + j for j in range(take)]
            block = jnp.concatenate(
                [
                    queries[:, :, h * head_size : (h + 1) * head_size].reshape(rows, head_size)
                    for h in heads
                ],
                axis=0,
            )
            scores = lax.dot_general(
                block, kept, (((1,), (1,)), ((), ())), preferred_element_type=jnp.float32
            )
            highest = jnp.max(scores, axis=1, keepdims=True)
            weights = jnp.exp2((scores - highest) * factor).astype(jnp.bfloat16)
            summed = jnp.dot(weights, value, preferred_element_type=jnp.float32)
            total = summed[:, head_size:]
            result = (summed[:, :head_size] / total).astype(jnp.bfloat16)
            lse = highest * scale + jnp.log(total)
            for j, h in enumerate(heads):
                out[:, :, h * head_size : (h + 1) * head_size] = result[
                    j * rows : (j + 1) * rows
                ].reshape(sources, count, head_size)
                lse_all = jnp.where(lane % local_heads == h, lse[j * rows : (j + 1) * rows], lse_all)
            start += take
    high = lse_all.astype(jnp.bfloat16).astype(jnp.float32)
    middle = (lse_all - high).astype(jnp.bfloat16).astype(jnp.float32)
    low = lse_all - high - middle
    piece = jnp.where(lane < local_heads, high, jnp.where(lane < 2 * local_heads, middle, low))
    width = local_heads * head_size
    out[:, :, width : width + LANES] = piece.astype(jnp.bfloat16).reshape(sources, count, LANES)


def attend_images(incoming, image_keys, image_values, image_lengths, group, scale):
    sources, held, count, width = incoming.shape
    if count % 16:
        incoming = incoming.transpose(1, 0, 2, 3).reshape(1, held, sources * count, width)
    lead, _, inner, _ = incoming.shape
    _, local_kv, tokens, head_size = image_keys.shape
    wide = width + LANES
    cache = pl.BlockSpec((None, local_kv, tokens, head_size), lambda i: (i, 0, 0, 0))
    out = pl.pallas_call(
        functools.partial(image_body, group=group, scale=scale),
        grid=(held,),
        in_specs=[
            pl.BlockSpec(memory_space=pltpu.SMEM),
            pl.BlockSpec((lead, None, inner, width), lambda i: (0, i, 0, 0)),
            cache,
            cache,
        ],
        out_specs=pl.BlockSpec((lead, None, inner, wide), lambda i: (0, i, 0, 0)),
        out_shape=jax.ShapeDtypeStruct((lead, held, inner, wide), jnp.bfloat16),
        compiler_params=pltpu.CompilerParams(vmem_limit_bytes=32 * 1024 * 1024),
        name="image_attention",
    )(image_lengths, incoming, image_keys, image_values)
    if count % 16:
        out = out.reshape(held, sources, count, wide).transpose(1, 0, 2, 3)
    return out


def prepare_body(request_image, image_slot, queries, outgoing, targets, *, most):
    local_heads, rows, _ = queries.shape
    images = image_slot.shape[0]
    chosen = request_image[...]
    slots = jnp.zeros((1, rows), jnp.int32)
    for image in range(images):
        slots = jnp.where(chosen == image, image_slot[image], slots)
    hits = jnp.where(lax.broadcasted_iota(jnp.int32, (images, rows), 0) == slots, 1.0, 0.0)
    earlier = lax.broadcasted_iota(jnp.int32, (rows, rows), 0) < lax.broadcasted_iota(
        jnp.int32, (rows, rows), 1
    )
    before = jnp.dot(
        hits.astype(jnp.bfloat16),
        jnp.where(earlier, 1.0, 0.0).astype(jnp.bfloat16),
        preferred_element_type=jnp.float32,
    )
    ranks = jnp.sum(hits * before, axis=0, keepdims=True)
    places = slots * most + ranks.astype(jnp.int32)
    targets[...] = places
    lines = lax.broadcasted_iota(jnp.int32, (images * most, rows), 0)
    dispatch = jnp.where(lines == places, 1.0, 0.0).astype(jnp.bfloat16)
    flat = jnp.concatenate([queries[h] for h in range(local_heads)], axis=1)
    outgoing[...] = jnp.dot(dispatch, flat, preferred_element_type=jnp.float32).astype(jnp.bfloat16)


def prepare(request_image, image_slot, queries, most):
    rows, local_heads, head_size = queries.shape
    images = image_slot.shape[0]
    return pl.pallas_call(
        functools.partial(prepare_body, most=most),
        out_shape=(
            jax.ShapeDtypeStruct((images * most, local_heads * head_size), jnp.bfloat16),
            jax.ShapeDtypeStruct((1, rows), jnp.int32),
        ),
        in_specs=[
            pl.BlockSpec(memory_space=pltpu.VMEM),
            pl.BlockSpec(memory_space=pltpu.SMEM),
            pl.BlockSpec(memory_space=pltpu.VMEM),
        ],
        compiler_params=pltpu.CompilerParams(vmem_limit_bytes=16 * 1024 * 1024),
        name="prepare",
    )(request_image.reshape(1, rows), image_slot, queries.transpose(1, 0, 2))


def merge_body(targets, back, text, text_lse, out):
    local_heads, rows, head_size = out.shape
    places = back.shape[0]
    width = local_heads * head_size
    lines = lax.broadcasted_iota(jnp.int32, (places, rows), 0)
    dispatch = jnp.where(lines == targets[...], 1.0, 0.0).astype(jnp.bfloat16)
    across = (((0,), (0,)), ((), ()))
    pieces = lax.dot_general(dispatch, back[:, width:], across, preferred_element_type=jnp.float32)
    source = lax.broadcasted_iota(jnp.int32, (LANES, LANES), 0)
    target = lax.broadcasted_iota(jnp.int32, (LANES, LANES), 1)
    joined = (source == target) & (target < local_heads)
    for piece in range(1, PIECES):
        joined = joined | ((source == target + piece * local_heads) & (target < local_heads))
    image_lse = jnp.dot(
        pieces.astype(jnp.bfloat16),
        jnp.where(joined, 1.0, 0.0).astype(jnp.bfloat16),
        preferred_element_type=jnp.float32,
    )[:, :local_heads]
    upper = jnp.maximum(image_lse, text_lse[...])
    image_weight = jnp.exp(image_lse - upper)
    share = image_weight / (image_weight + jnp.exp(text_lse[...] - upper))
    image = lax.dot_general(dispatch, back[:, :width], across, preferred_element_type=jnp.float32)
    for h in range(local_heads):
        own = text[h]
        part = image[:, h * head_size : (h + 1) * head_size]
        out[h] = (own + share[:, h : h + 1] * (part - own)).astype(jnp.bfloat16)


def merge(targets, back, text, text_lse, local_heads):
    rows = targets.shape[1]
    head_size = text.shape[2]
    return pl.pallas_call(
        merge_body,
        out_shape=jax.ShapeDtypeStruct((local_heads, rows, head_size), jnp.bfloat16),
        compiler_params=pltpu.CompilerParams(vmem_limit_bytes=16 * 1024 * 1024),
        name="merge",
    )(targets, back, text, text_lse).transpose(1, 0, 2)


def on_device(
    queries,
    request_image,
    image_slot,
    image_lengths,
    image_keys,
    image_values,
    text_keys,
    text_values,
    text_lengths,
):
    rows, local_heads, head_size = queries.shape
    local_kv = image_keys.shape[1]
    group = local_heads // local_kv
    images = image_slot.shape[0]
    held = image_keys.shape[0]
    image_tokens = image_keys.shape[2]
    text_tokens = text_keys.shape[2]
    devices = lax.axis_size("seq")
    most = max(2, 2 * rows // images)
    width = local_heads * head_size
    scale = 1.0 / math.sqrt(head_size)
    outgoing, targets = prepare(request_image, image_slot, queries, most)
    outgoing = outgoing.reshape(devices, held, most, width)
    incoming = lax.all_to_all(outgoing, "seq", split_axis=0, concat_axis=0, tiled=True)
    heads = queries.reshape(rows, local_kv, group, head_size)
    scores = (
        jnp.einsum("rhgd,rhtd->rhgt", heads, text_keys, preferred_element_type=jnp.float32) * scale
    )
    valid = (jnp.arange(text_tokens, dtype=jnp.int32)[None, :] < text_lengths[:, None])[
        :, None, None, :
    ]
    weights, total, highest = weigh(scores, valid)
    text_out = (
        jnp.einsum("rhgt,rhtd->rhgd", weights, text_values, preferred_element_type=jnp.float32)
        / total
    )
    text_lse = highest[..., 0] + jnp.log(total[..., 0])
    text_flat = text_out.reshape(rows, local_heads, head_size).transpose(1, 0, 2)
    text_lse = text_lse.reshape(rows, local_heads)
    incoming, text_flat, text_lse = lax.optimization_barrier((incoming, text_flat, text_lse))
    stacked = attend_images(incoming, image_keys, image_values, image_lengths, group, scale)
    back = lax.all_to_all(stacked, "seq", split_axis=0, concat_axis=0, tiled=True)
    flat_back = back.reshape(images * most, width + LANES)
    return merge(targets, flat_back, text_flat, text_lse, local_heads)


def solution(mesh):
    in_specs = (
        P(("groups", "seq"), "head", None),
        P(("groups", "seq"), None),
        P("groups"),
        P(("groups", "seq")),
        P(("groups", "seq"), "head", None, None),
        P(("groups", "seq"), "head", None, None),
        P(("groups", "seq"), "head", None, None),
        P(("groups", "seq"), "head", None, None),
        P(("groups", "seq")),
    )
    out_specs = P(("groups", "seq"), "head", None)
    return jax.shard_map(
        on_device, mesh=mesh, in_specs=in_specs, out_specs=out_specs, check_vma=False
    )
```
